8 devices in a mesh: dp: 1 (over z), tp: 8 (over y, x, core).
Axes of the slice: x: 2, y: 2, z: 1, core: 2. Of those that a mesh axis runs over, the one named last changes fastest.
Arguments:
- x: bfloat16 [8192, 3072], P('dp')
- pos: int32 [8192], P('dp')
- g1: bfloat16 [3072], replicated
- g2: bfloat16 [3072], replicated
- wq: bfloat16 [3072, 3072], P(None, 'tp')
- wk: bfloat16 [3072, 1024], replicated
- wv: bfloat16 [3072, 1024], replicated
- wo: bfloat16 [3072, 3072], P('tp')
- wg: bfloat16 [3072, 8192], P(None, 'tp')
- wu: bfloat16 [3072, 8192], P(None, 'tp')
- wd: bfloat16 [8192, 3072], P('tp')
Outputs:
- output 1: bfloat16 [8192, 3072], P('dp')
- output 2: bfloat16 [8192, 8, 128], P('dp', 'tp')
- output 3: bfloat16 [8192, 8, 128], P('dp', 'tp')
All inputs are finite; a program needn't handle non-finite values.
Results may differ from the reference program's by a relative error of at most 0.0156133.
Values are sent between devices in bfloat16 or wider.
A program may use at most 1 GiB of HBM per device.

```python
import jax
import jax.numpy as jnp
from jax import lax
import numpy as np

D = 3072
HEADS = 24
KV_HEADS = 8
HEAD = 128
FF = 8192
T = 8192
SLOTS = 8

EPS = 1e-5
ROPE_BASE = 500000.0
R = HEADS // KV_HEADS
QB = min(T, 256)


def setup_inputs(seed: int = 0, part: int = 0) -> dict:
    base = jax.random.PRNGKey(seed)
    kw = jax.random.split(jax.random.fold_in(base, 0), 9)
    kx, kp = jax.random.split(jax.random.fold_in(jax.random.fold_in(base, 1), part))

    def w(k, shape, scale):
        return (jax.random.normal(k, shape, jnp.float32) * scale).astype(jnp.bfloat16)

    def gain(k):
        return (1.0 + 0.2 * jax.random.normal(k, (D,), jnp.float32)).astype(jnp.bfloat16)

    x = jax.random.normal(kx, (T, D), jnp.float32).astype(jnp.bfloat16)
    pos = jax.random.randint(kp, (), 0, 4096, dtype=jnp.int32) + jnp.arange(T, dtype=jnp.int32)
    return {
        "x": x,
        "pos": pos,
        "g1": gain(kw[0]),
        "g2": gain(kw[1]),
        "wq": w(kw[2], (D, HEADS * HEAD), 1.5 * D ** -0.5),
        "wk": w(kw[3], (D, KV_HEADS * HEAD), 1.5 * D ** -0.5),
        "wv": w(kw[4], (D, KV_HEADS * HEAD), D ** -0.5),
        "wo": w(kw[5], (HEADS * HEAD, D), 2.0 * (HEADS * HEAD) ** -0.5),
        "wg": w(kw[6], (D, FF), D ** -0.5),
        "wu": w(kw[7], (D, FF), D ** -0.5),
        "wd": w(kw[8], (FF, D), 2.0 * FF ** -0.5),
    }


def _rms(x, g):
    x32 = x.astype(jnp.float32)
    inv = lax.rsqrt(jnp.mean(x32 * x32, axis=-1, keepdims=True) + EPS)
    return (x32 * inv * g.astype(jnp.float32)).astype(jnp.bfloat16)


def _rope(t, pos):
    half = HEAD // 2
    inv = ROPE_BASE ** (-2.0 * jnp.arange(half, dtype=jnp.float32) / HEAD)
    ang = pos.astype(jnp.float32)[:, None] * inv[None, :]
    c = jnp.cos(ang)[:, None, :]
    s = jnp.sin(ang)[:, None, :]
    t1, t2 = t[..., :half], t[..., half:]
    return jnp.concatenate([t1 * c - t2 * s, t2 * c + t1 * s], axis=-1)


def reference(x, pos, g1, g2, wq, wk, wv, wo, wg, wu, wd):
    a = _rms(x, g1)
    q = _rope(jnp.dot(a, wq, preferred_element_type=jnp.float32).reshape(T, HEADS, HEAD), pos).astype(jnp.bfloat16)
    k = _rope(jnp.dot(a, wk, preferred_element_type=jnp.float32).reshape(T, KV_HEADS, HEAD), pos).astype(jnp.bfloat16)
    v = jnp.dot(a, wv, preferred_element_type=jnp.float32).astype(jnp.bfloat16).reshape(T, KV_HEADS, HEAD)
    qg = q.reshape(T // QB, QB, KV_HEADS, R, HEAD)
    pq = pos.reshape(T // QB, QB)
    scale = HEAD ** -0.5

    def one_head(g):
        kg = k[:, g].astype(jnp.float32)
        vg = v[:, g].astype(jnp.float32)

        def one_block(blk):
            qq, pb = blk
            sc = jnp.einsum("qrd,kd->rqk", qq.astype(jnp.float32), kg) * scale
            sc = jnp.where((pos[None, :] <= pb[:, None])[None], sc, -jnp.inf)
            e = jnp.exp(sc - jnp.max(sc, axis=-1, keepdims=True))
            pr = (e / jnp.sum(e, axis=-1, keepdims=True)).astype(jnp.bfloat16)
            return jnp.einsum("rqk,kd->qrd", pr.astype(jnp.float32), vg).astype(jnp.bfloat16)

        return lax.map(one_block, (qg[:, :, g], pq))

    o = lax.map(one_head, jnp.arange(KV_HEADS))
    o = o.transpose(1, 2, 0, 3, 4).reshape(T, HEADS * HEAD)
    h = (x.astype(jnp.float32) + jnp.dot(o, wo, preferred_element_type=jnp.float32)).astype(jnp.bfloat16)
    b = _rms(h, g2)
    gt = jnp.dot(b, wg, preferred_element_type=jnp.float32)
    up = jnp.dot(b, wu, preferred_element_type=jnp.float32)
    u = (jax.nn.silu(gt) * up).astype(jnp.bfloat16)
    y = (h.astype(jnp.float32) + jnp.dot(u, wd, preferred_element_type=jnp.float32)).astype(jnp.bfloat16)
    sl = np.arange(SLOTS) * KV_HEADS // SLOTS
    return (y, k[:, sl], v[:, sl])
```

```python
import functools

import jax
import jax.numpy as jnp
from jax import lax
from jax.experimental import pallas as pl
from jax.experimental.pallas import tpu as pltpu
from jax.sharding import PartitionSpec as P

HEAD = 128
EPS = 1e-5
ROPE_BASE = 500000.0
LOG2E = 1.4426950408889634
CHUNKS = 4
F32, BF = jnp.float32, jnp.bfloat16


def _cs(pos):
    half = HEAD // 2
    inv = ROPE_BASE ** (-2.0 * jnp.arange(half, dtype=F32) / HEAD)
    ang = pos.astype(F32)[:, None] * inv
    return jnp.cos(ang), jnp.sin(ang)


def _qkv_kernel(hl, x_ref, g_ref, w_ref, c_ref, s_ref, q_ref, k_ref, v_ref):
    x = x_ref[...].astype(F32)
    inv = lax.rsqrt(jnp.mean(x * x, axis=-1, keepdims=True) + EPS)
    a = (x * inv * g_ref[...].astype(F32)).astype(BF)
    r = jnp.dot(a, w_ref[...], preferred_element_type=F32)
    c, s = c_ref[...], s_ref[...]
    cc = jnp.concatenate([c, c], axis=-1)
    ss = jnp.concatenate([-s, s], axis=-1)
    for n in range(hl + 1):
        t = r[:, n * HEAD:(n + 1) * HEAD]
        t = (t * cc + pltpu.roll(t, HEAD // 2, 1) * ss).astype(BF)
        if n < hl:
            q_ref[:, n * HEAD:(n + 1) * HEAD] = t
        else:
            k_ref[...] = t
    v_ref[...] = r[:, (hl + 1) * HEAD:].astype(BF)


def _qkv(x, g1, w, c, s, hl):
    t, d = x.shape
    bm = min(t, 512)
    n = w.shape[1]
    row = lambda i: (i, 0)
    fix = lambda i: (0, 0)
    return pl.pallas_call(
        functools.partial(_qkv_kernel, hl),
        grid=(t // bm,),
        in_specs=[
            pl.BlockSpec((bm, d), row),
            pl.BlockSpec((1, d), fix),
            pl.BlockSpec((d, n), fix),
            pl.BlockSpec((bm, HEAD // 2), row),
            pl.BlockSpec((bm, HEAD // 2), row),
        ],
        out_specs=[
            pl.BlockSpec((bm, hl * HEAD), row),
            pl.BlockSpec((bm, HEAD), row),
            pl.BlockSpec((bm, HEAD), row),
        ],
        out_shape=[
            jax.ShapeDtypeStruct((t, hl * HEAD), BF),
            jax.ShapeDtypeStruct((t, HEAD), BF),
            jax.ShapeDtypeStruct((t, HEAD), BF),
        ],
        compiler_params=pltpu.CompilerParams(vmem_limit_bytes=56 << 20),
        cost_estimate=pl.CostEstimate(flops=2 * t * d * n, bytes_accessed=2 * t * d, transcendentals=0),
        name="qkv",
    )(x, g1.reshape(1, d), w, c, s)


def _attn_kernel(hl, q0, bq, bk, q_ref, kt_ref, v_ref, o_ref, m_sc, l_sc, a_sc):
    i = pl.program_id(0)
    row0 = q0 + i * bq
    c = HEAD ** -0.5 * LOG2E
    for h in range(hl):
        m_sc[h] = jnp.full((bq, HEAD), -1e30, F32)
        l_sc[h] = jnp.zeros((bq, HEAD), F32)
        a_sc[h] = jnp.zeros((bq, HEAD), F32)

    def block(j, masked):
        start = pl.multiple_of(j * bk, bk)
        kt = kt_ref[:, pl.ds(start, bk)]
        v = v_ref[pl.ds(start, bk), :]
        for h in range(hl):
            q = q_ref[:, h * HEAD:(h + 1) * HEAD]
            s = jnp.dot(q, kt, preferred_element_type=F32) * c
            if masked:
                rows = row0 + lax.broadcasted_iota(jnp.int32, (bq, bk), 0)
                cols = start + lax.broadcasted_iota(jnp.int32, (bq, bk), 1)
                s = jnp.where(cols <= rows, s, -jnp.inf)
            m0 = m_sc[h]
            m1 = jnp.maximum(m0, jnp.max(s, axis=-1, keepdims=True))
            p = jnp.exp2(s - jnp.concatenate([m1] * (bk // HEAD), axis=-1))
            al = jnp.exp2(m0 - m1)
            part = p[:, :HEAD]
            for g in range(1, bk // HEAD):
                part = part + p[:, g * HEAD:(g + 1) * HEAD]
            l_sc[h] = l_sc[h] * al + part
            a_sc[h] = a_sc[h] * al + jnp.dot(p.astype(BF), v, preferred_element_type=F32)
            m_sc[h] = m1

    nfull = row0 // bk

    def body(j, carry):
        block(j, False)
        return carry

    lax.fori_loop(0, nfull, body, 0)
    block(nfull, True)
    for h in range(hl):
        l = jnp.sum(l_sc[h], axis=-1, keepdims=True)
        o_ref[:, h * HEAD:(h + 1) * HEAD] = (a_sc[h] / l).astype(BF)


def _attn(q, kt, v, hl, chunk, rows):
    t = v.shape[0]
    bq = min(rows, 512)
    bk = bq
    nq = rows // bq
    b0 = chunk * nq
    end = (chunk + 1) * rows
    area = sum((chunk * rows + (i + 1) * bq) * bq for i in range(nq))
    return pl.pallas_call(
        functools.partial(_attn_kernel, hl, chunk * rows, bq, bk),
        grid=(nq,),
        in_specs=[
            pl.BlockSpec((bq, hl * HEAD), lambda i: (b0 + i, 0)),
            pl.BlockSpec((HEAD, t), lambda i: (0, 0)),
            pl.BlockSpec((t, HEAD), lambda i: (0, 0)),
        ],
        out_specs=pl.BlockSpec((bq, hl * HEAD), lambda i: (i, 0)),
        out_shape=jax.ShapeDtypeStruct((rows, hl * HEAD), BF),
        scratch_shapes=[pltpu.VMEM((hl, bq, HEAD), F32)] * 3,
        compiler_params=pltpu.CompilerParams(vmem_limit_bytes=40 << 20),
        cost_estimate=pl.CostEstimate(
            flops=4 * 3 * HEAD * hl * area, bytes_accessed=4 * end * HEAD, transcendentals=hl * area),
        name=f"attn{chunk}",
    )(q, kt, v)


def _h_kernel(n, off_ref, x_ref, g_ref, *refs):
    o_refs, w_ref, h_ref, b_ref = refs[:n], refs[n], refs[n + 1], refs[n + 2]
    o = jnp.concatenate([r[...] for r in o_refs], axis=-1)
    h = (x_ref[...].astype(F32) + jnp.dot(o, w_ref[...], preferred_element_type=F32)).astype(BF)
    h_ref[...] = h
    h = h.astype(F32)
    inv = lax.rsqrt(jnp.mean(h * h, axis=-1, keepdims=True) + EPS)
    b_ref[...] = (h * inv * g_ref[...].astype(F32)).astype(BF)


def _h(off, x, g2, os, wo, chunk):
    rows, kk = os[0].shape
    d = x.shape[1]
    n = len(os)
    bm = min(rows, 256)
    nb = rows // bm
    row = lambda i, o: (i, 0)
    fix = lambda i, o: (0, 0)
    return pl.pallas_call(
        functools.partial(_h_kernel, n),
        grid_spec=pltpu.PrefetchScalarGridSpec(
            num_scalar_prefetch=1,
            grid=(nb,),
            in_specs=[
                pl.BlockSpec((bm, d), lambda i, o: (o[0] * nb + i, 0)),
                pl.BlockSpec((1, d), fix),
                *[pl.BlockSpec((bm, kk), row) for _ in range(n)],
                pl.BlockSpec((n * kk, d), fix, pipeline_mode=pl.Buffered(1)),
            ],
            out_specs=[pl.BlockSpec((bm, d), row), pl.BlockSpec((bm, d), row)],
        ),
        out_shape=[jax.ShapeDtypeStruct((rows, d), BF)] * 2,
        compiler_params=pltpu.CompilerParams(vmem_limit_bytes=58 << 20),
        cost_estimate=pl.CostEstimate(
            flops=2 * rows * d * n * kk, bytes_accessed=2 * d * (n * kk + 4 * rows), transcendentals=0),
        name=f"h{chunk}",
    )(off, x, g2.reshape(1, d), *os, wo)


def _mlp_kernel(nb, fb, db, b0_ref, b1_ref, wg_ref, wu_ref, wd_ref, p0_ref, p1_ref, u_sc):
    i = pl.program_id(0)
    b = jnp.where(i < nb, b0_ref[...], b1_ref[...])
    for f in range(0, wg_ref.shape[1], fb):
        gt = jnp.dot(b, wg_ref[:, f:f + fb], preferred_element_type=F32)
        up = jnp.dot(b, wu_ref[:, f:f + fb], preferred_element_type=F32)
        u_sc[:, f:f + fb] = (gt * jax.nn.sigmoid(gt) * up).astype(BF)
    u = u_sc[...]

    def down(p_ref):
        for n in range(0, wd_ref.shape[1], db):
            p_ref[:, n:n + db] = jnp.dot(u, wd_ref[:, n:n + db], preferred_element_type=F32).astype(BF)

    @pl.when(i < nb)
    def _():
        down(p0_ref)

    @pl.when(i >= nb)
    def _():
        down(p1_ref)


def _mlp(b0, b1, wg, wu, wd, chunk):
    rows, d = b0.shape
    f = wg.shape[1]
    bm = min(rows, 512)
    nb = rows // bm
    first = lambda i: (jnp.minimum(i, nb - 1), 0)
    second = lambda i: (jnp.maximum(i - nb, 0), 0)
    fix = lambda i: (0, 0)
    one = pl.Buffered(1)
    return pl.pallas_call(
        functools.partial(_mlp_kernel, nb, min(f, 512), min(d, 512)),
        grid=(2 * nb,),
        in_specs=[
            pl.BlockSpec((bm, d), first),
            pl.BlockSpec((bm, d), second),
            pl.BlockSpec((d, f), fix, pipeline_mode=one),
            pl.BlockSpec((d, f), fix, pipeline_mode=one),
            pl.BlockSpec((f, d), fix, pipeline_mode=one),
        ],
        out_specs=[pl.BlockSpec((bm, d), first), pl.BlockSpec((bm, d), second)],
        out_shape=[jax.ShapeDtypeStruct((rows, d), BF)] * 2,
        scratch_shapes=[pltpu.VMEM((bm, f), BF)],
        compiler_params=pltpu.CompilerParams(vmem_limit_bytes=62 << 20),
        cost_estimate=pl.CostEstimate(
            flops=12 * rows * d * f, bytes_accessed=2 * d * (3 * f + 4 * rows), transcendentals=2 * rows * f),
        name=f"mlp{chunk}",
    )(b0, b1, wg, wu, wd)


def solution(mesh):
    tp = mesh.shape["tp"]
    assert tp == 8

    def swap(a, bit):
        return lax.ppermute(a, "tp", [(i, i ^ bit) for i in range(tp)])

    core, xs, ys = 1, 2, 4

    def local(x, pos, g1, g2, wq, wk, wv, wo, wg, wu, wd):
        t, d = x.shape
        hl = wq.shape[1] // HEAD
        r = lax.axis_index("tp")
        c, q4 = r % 2, r // 2
        rows = t // CHUNKS
        half, piece = rows // 2, rows // 8

        m = wo.shape[0] // 2
        w2, w4 = swap(wo, xs), swap(wo, ys)
        w6a, w6b = swap(w2[:m], ys), swap(w4[m:], xs)
        ws = [wo, w2, w4, w6a, w6b]
        wp = [swap(w, core) for w in ws]
        wo_all = jnp.concatenate(
            [ws[0], wp[0], ws[1], wp[1], ws[2], wp[2], ws[3], ws[4], wp[3], wp[4]], axis=0)

        wk_l = lax.dynamic_slice_in_dim(wk, r * HEAD, HEAD, axis=1)
        wv_l = lax.dynamic_slice_in_dim(wv, r * HEAD, HEAD, axis=1)
        cos, sin = _cs(pos)
        q, k, v = _qkv(x, g1, jnp.concatenate([wq, wk_l, wv_l], axis=1), cos, sin, hl)
        kt = k.T

        y = jnp.zeros((t, d), BF)
        for n in range(CHUNKS):
            o = _attn(q, kt, v, hl, n, rows)
            oa = lax.dynamic_slice_in_dim(o, c * half, half, axis=0)
            ob = swap(lax.dynamic_slice_in_dim(o, (1 - c) * half, half, axis=0), core)
            oax, obx = swap(oa, xs), swap(ob, xs)
            oay, oby = swap(oa, ys), swap(ob, ys)
            oad, obd = swap(oax, ys), swap(oby, xs)
            h, b = _h((2 * n + c).reshape(1), x, g2, [oa, ob, oax, obx, oay, oby, oad, obd], wo_all, n)
            p0, p1 = _mlp(b, swap(b, core), wg, wu, wd, n)
            p1 = swap(p1, core)

            def part(a, k, lo=0, hi=piece):
                return lax.dynamic_slice_in_dim(a, (q4 ^ k) * piece + lo, hi - lo, axis=0).astype(F32)

            hp = piece // 2
            fx = swap((part(p0, 3, 0, hp) + part(p1, 3, 0, hp)).astype(BF), xs)
            fy = swap((part(p0, 3, hp) + part(p1, 3, hp)).astype(BF), ys)
            sya = part(p0, 2, 0, hp) + part(p1, 2, 0, hp) + fx.astype(F32)
            syb = part(p0, 2, hp) + part(p1, 2, hp)
            sxa = part(p0, 1, 0, hp) + part(p1, 1, 0, hp)
            sxb = part(p0, 1, hp) + part(p1, 1, hp) + fy.astype(F32)
            gya, gyb = swap(sya.astype(BF), ys), swap(syb.astype(BF), ys)
            gxa, gxb = swap(sxa.astype(BF), xs), swap(sxb.astype(BF), xs)
            ya = (part(h, 0, 0, hp) + (part(p0, 0, 0, hp) + part(p1, 0, 0, hp)
                                       + gya.astype(F32) + gxa.astype(F32))).astype(BF)
            yb = (part(h, 0, hp) + (part(p0, 0, hp) + part(p1, 0, hp)
                                    + gyb.astype(F32) + gxb.astype(F32))).astype(BF)
            yax, ybx = swap(ya, xs), swap(yb, xs)
            yay, yby = swap(ya, ys), swap(yb, ys)
            yad, ybd = swap(yax, ys), swap(yby, xs)
            for kk, (u, w) in enumerate(((ya, yb), (yax, ybx), (yay, yby), (yad, ybd))):
                at = n * rows + (q4 ^ kk) * piece
                for lo, s in ((0, u), (hp, w)):
                    y = lax.dynamic_update_slice_in_dim(y, s, at + c * half + lo, axis=0)
                    y = lax.dynamic_update_slice_in_dim(y, swap(s, core), at + (1 - c) * half + lo, axis=0)
        return y, k.reshape(t, 1, HEAD), v.reshape(t, 1, HEAD)

    return jax.shard_map(
        local,
        mesh=mesh,
        in_specs=(P("dp", None), P("dp"), P(), P(), P(None, "tp"), P(), P(), P("tp", None),
                  P(None, "tp"), P(None, "tp"), P("tp", None)),
        out_specs=(P("dp", None), P("dp", "tp", None), P("dp", "tp", None)),
        check_vma=False,
    )
```

```python
import functools

import jax
import jax.numpy as jnp
from jax import lax
from jax.experimental import pallas as pl
from jax.experimental.pallas import tpu as pltpu
from jax.sharding import PartitionSpec as P


HEAD = 128
EPS = 1e-5
ROPE_BASE = 500000.0
LOG2E = 1.4426950408889634
CHUNKS = (2048, 1536, 2048, 1536, 1024)
VMEM = 62 << 20
F32, BF = jnp.float32, jnp.bfloat16


def _cs(pos):
    half = HEAD // 2
    inv = ROPE_BASE ** (-2.0 * jnp.arange(half, dtype=F32) / HEAD)
    ang = pos.astype(F32)[:, None] * inv
    return jnp.cos(ang), jnp.sin(ang)


def _qkv_kernel(hl, x_ref, g_ref, w_ref, c_ref, s_ref, q_ref, k_ref, v_ref):
    x = x_ref[...].astype(F32)
    inv = lax.rsqrt(jnp.mean(x * x, axis=-1, keepdims=True) + EPS)
    a = (x * inv * g_ref[...].astype(F32)).astype(BF)
    r = jnp.dot(a, w_ref[...], preferred_element_type=F32)
    c, s = c_ref[...], s_ref[...]
    cc = jnp.concatenate([c, c], axis=-1)
    ss = jnp.concatenate([-s, s], axis=-1)
    for n in range(hl + 1):
        t = r[:, n * HEAD:(n + 1) * HEAD]
        t = (t * cc + pltpu.roll(t, HEAD // 2, 1) * ss).astype(BF)
        if n < hl:
            q_ref[:, n * HEAD:(n + 1) * HEAD] = t
        else:
            k_ref[...] = t
    v_ref[...] = r[:, (hl + 1) * HEAD:].astype(BF)


def _qkv(x, g1, w, c, s, hl):
    t, d = x.shape
    bm = min(t, 512)
    n = w.shape[1]
    row = lambda i: (i, 0)
    fix = lambda i: (0, 0)
    return pl.pallas_call(
        functools.partial(_qkv_kernel, hl),
        grid=(t // bm,),
        in_specs=[
            pl.BlockSpec((bm, d), row),
            pl.BlockSpec((1, d), fix),
            pl.BlockSpec((d, n), fix),
            pl.BlockSpec((bm, HEAD // 2), row),
            pl.BlockSpec((bm, HEAD // 2), row),
        ],
        out_specs=[
            pl.BlockSpec((bm, hl * HEAD), row),
            pl.BlockSpec((bm, HEAD), row),
            pl.BlockSpec((bm, HEAD), row),
        ],
        out_shape=[
            jax.ShapeDtypeStruct((t, hl * HEAD), BF),
            jax.ShapeDtypeStruct((t, HEAD), BF),
            jax.ShapeDtypeStruct((t, HEAD), BF),
        ],
        compiler_params=pltpu.CompilerParams(vmem_limit_bytes=VMEM),
        cost_estimate=pl.CostEstimate(flops=2 * t * d * n, bytes_accessed=2 * t * d, transcendentals=0),
        name="qkv",
    )(x, g1.reshape(1, d), w, c, s)


def _attn_kernel(hl, q0, bq, bk, q_ref, kt_ref, v_ref, o_ref, m_sc, l_sc, a_sc):
    i = pl.program_id(0)
    row0 = q0 + i * bq
    c = HEAD ** -0.5 * LOG2E
    for h in range(hl):
        m_sc[h] = jnp.full((bq, HEAD), -1e30, F32)
        l_sc[h] = jnp.zeros((bq, HEAD), F32)
        a_sc[h] = jnp.zeros((bq, HEAD), F32)

    def block(j, masked):
        start = pl.multiple_of(j * bk, bk)
        kt = kt_ref[:, pl.ds(start, bk)]
        v = v_ref[pl.ds(start, bk), :]
        scores = []
        for h in range(hl):
            q = q_ref[:, h * HEAD:(h + 1) * HEAD]
            s = jnp.dot(q, kt, preferred_element_type=F32) * c
            if masked:
                rows = row0 + lax.broadcasted_iota(jnp.int32, (bq, bk), 0)
                cols = start + lax.broadcasted_iota(jnp.int32, (bq, bk), 1)
                s = jnp.where(cols <= rows, s, -jnp.inf)
            scores.append(s)
        for h in range(hl):
            s = scores[h]
            m0 = m_sc[h]
            m1 = jnp.maximum(m0, jnp.max(s, axis=-1, keepdims=True))
            p = jnp.exp2(s - jnp.concatenate([m1] * (bk // HEAD), axis=-1))
            al = jnp.exp2(m0 - m1)
            part = p[:, :HEAD]
            for g in range(1, bk // HEAD):
                part = part + p[:, g * HEAD:(g + 1) * HEAD]
            l_sc[h] = l_sc[h] * al + part
            a_sc[h] = a_sc[h] * al + jnp.dot(p.astype(BF), v, preferred_element_type=F32)
            m_sc[h] = m1

    nfull = row0 // bk

    def body(j, carry):
        block(j, False)
        return carry

    lax.fori_loop(0, nfull, body, 0)
    block(nfull, True)
    for h in range(hl):
        l = jnp.sum(l_sc[h], axis=-1, keepdims=True)
        o_ref[:, h * HEAD:(h + 1) * HEAD] = (a_sc[h] / l).astype(BF)


def _attn(q, kt, v, hl, q0, rows):
    t = v.shape[0]
    bq = min(rows, 512)
    bk = bq
    nq = rows // bq
    b0 = q0 // bq
    end = q0 + rows
    area = sum((q0 + (i + 1) * bq) * bq for i in range(nq))
    return pl.pallas_call(
        functools.partial(_attn_kernel, hl, q0, bq, bk),
        grid=(nq,),
        in_specs=[
            pl.BlockSpec((bq, hl * HEAD), lambda i: (b0 + i, 0)),
            pl.BlockSpec((HEAD, t), lambda i: (0, 0)),
            pl.BlockSpec((t, HEAD), lambda i: (0, 0)),
        ],
        out_specs=pl.BlockSpec((bq, hl * HEAD), lambda i: (i, 0)),
        out_shape=jax.ShapeDtypeStruct((rows, hl * HEAD), BF),
        scratch_shapes=[pltpu.VMEM((hl, bq, HEAD), F32)] * 3,
        compiler_params=pltpu.CompilerParams(vmem_limit_bytes=VMEM),
        cost_estimate=pl.CostEstimate(
            flops=4 * 3 * HEAD * hl * area, bytes_accessed=4 * end * HEAD, transcendentals=hl * area),
    )(q, kt, v)


def _h_kernel(n, sizes, off_ref, x_ref, g_ref, *refs):
    o_refs, w_refs = refs[:n], refs[n:n + len(sizes)]
    h_ref, b_ref, w_sc, sem = refs[n + len(sizes):]

    @pl.when(pl.program_id(0) == 0)
    def _():
        copies, at = [], 0
        for i, (w, size) in enumerate(zip(w_refs, sizes)):
            copies.append(pltpu.make_async_copy(w, w_sc.at[pl.ds(at, size), :], sem.at[i]))
            at += size
        for cp in copies:
            cp.start()
        for cp in copies:
            cp.wait()

    o = jnp.concatenate([r[...] for r in o_refs], axis=-1)
    h = (x_ref[...].astype(F32) + jnp.dot(o, w_sc[...], preferred_element_type=F32)).astype(BF)
    h_ref[...] = h
    h = h.astype(F32)
    inv = lax.rsqrt(jnp.mean(h * h, axis=-1, keepdims=True) + EPS)
    b_ref[...] = (h * inv * g_ref[...].astype(F32)).astype(BF)


def _h(start, x, g2, os, ws):
    rows, kk = os[0].shape
    d = x.shape[1]
    n = len(os)
    bm = min(rows, 256)
    sizes = tuple(w.shape[0] for w in ws)
    row = lambda i, o: (i, 0)
    fix = lambda i, o: (0, 0)
    return pl.pallas_call(
        functools.partial(_h_kernel, n, sizes),
        grid_spec=pltpu.PrefetchScalarGridSpec(
            num_scalar_prefetch=1,
            grid=(rows // bm,),
            in_specs=[
                pl.BlockSpec((bm, d), lambda i, o: (o[0] + i, 0)),
                pl.BlockSpec((1, d), fix),
                *[pl.BlockSpec((bm, kk), row) for _ in range(n)],
                *[pl.BlockSpec(memory_space=pl.ANY) for _ in ws],
            ],
            out_specs=[pl.BlockSpec((bm, d), row), pl.BlockSpec((bm, d), row)],
            scratch_shapes=[pltpu.VMEM((n * kk, d), BF), pltpu.SemaphoreType.DMA((len(ws),))],
        ),
        out_shape=[jax.ShapeDtypeStruct((rows, d), BF)] * 2,
        compiler_params=pltpu.CompilerParams(vmem_limit_bytes=VMEM),
        cost_estimate=pl.CostEstimate(
            flops=2 * rows * d * n * kk, bytes_accessed=2 * d * (n * kk + 4 * rows), transcendentals=0),
    )((start // bm).reshape(1), x, g2.reshape(1, d), *os, *ws)


def _mlp_kernel(fb, db, b_ref, wg_ref, wu_ref, wd_ref, p_ref, wg_sc, wu_sc, wd_sc, u_sc, sem):
    d, f = wg_sc.shape
    first = pl.program_id(0) == 0

    def up_copies(j):
        cols = pl.ds(j * fb, fb)
        return (pltpu.make_async_copy(wg_ref.at[:, cols], wg_sc.at[:, cols], sem.at[0, j]),
                pltpu.make_async_copy(wu_ref.at[:, cols], wu_sc.at[:, cols], sem.at[1, j]))

    def down_copy():
        return pltpu.make_async_copy(wd_ref, wd_sc, sem.at[2, 0])

    @pl.when(first)
    def _():
        for j in range(f // fb):
            for cp in up_copies(j):
                cp.start()
        down_copy().start()

    b = b_ref[...]
    for j in range(f // fb):
        @pl.when(first)
        def _():
            for cp in up_copies(j):
                cp.wait()

        cols = slice(j * fb, (j + 1) * fb)
        gt = jnp.dot(b, wg_sc[:, cols], preferred_element_type=F32)
        up = jnp.dot(b, wu_sc[:, cols], preferred_element_type=F32)
        u_sc[:, cols] = (gt * jax.nn.sigmoid(gt) * up).astype(BF)

    @pl.when(first)
    def _():
        down_copy().wait()

    u = u_sc[...]
    for j in range(d // db):
        cols = slice(j * db, (j + 1) * db)
        p_ref[:, cols] = jnp.dot(u, wd_sc[:, cols], preferred_element_type=F32).astype(BF)


def _mlp(b, wg, wu, wd):
    rows, d = b.shape
    f = wg.shape[1]
    bm = next((m for m in (512, 384, 256) if rows % m == 0), rows)
    fb, db = min(f, 512), min(d, 512)
    row = lambda i: (i, 0)
    any_ = pl.BlockSpec(memory_space=pl.ANY)
    return pl.pallas_call(
        functools.partial(_mlp_kernel, fb, db),
        grid=(rows // bm,),
        in_specs=[pl.BlockSpec((bm, d), row), any_, any_, any_],
        out_specs=pl.BlockSpec((bm, d), row),
        out_shape=jax.ShapeDtypeStruct((rows, d), BF),
        scratch_shapes=[pltpu.VMEM((d, f), BF), pltpu.VMEM((d, f), BF), pltpu.VMEM((f, d), BF),
                        pltpu.VMEM((bm, f), BF), pltpu.SemaphoreType.DMA((3, f // fb))],
        compiler_params=pltpu.CompilerParams(vmem_limit_bytes=VMEM),
        cost_estimate=pl.CostEstimate(
            flops=6 * rows * d * f, bytes_accessed=2 * d * (3 * f + 2 * rows), transcendentals=rows * f),
    )(b, wg, wu, wd)


def _sum_kernel(groups, q_ref, *refs):
    at = 0
    outs = refs[sum(groups):]
    for g, out in zip(groups, outs):
        t = refs[at][...].astype(F32)
        for r in refs[at + 1:at + g]:
            t = t + r[...].astype(F32)
        out[...] = t.astype(BF)
        at += g


def _sums(q4, piece, terms):
    d = terms[0][0][0].shape[1]
    bm = min(piece, 64)
    nb = piece // bm
    own = lambda i, q: (i, 0)

    def spec(k):
        if k is None:
            return pl.BlockSpec((bm, d), own)
        return pl.BlockSpec((bm, d), lambda i, q: (q[k] * nb + i, 0))

    flat = [t for group in terms for t in group]
    return pl.pallas_call(
        functools.partial(_sum_kernel, tuple(len(g) for g in terms)),
        grid_spec=pltpu.PrefetchScalarGridSpec(
            num_scalar_prefetch=1,
            grid=(nb,),
            in_specs=[spec(k) for _, k in flat],
            out_specs=[pl.BlockSpec((bm, d), own) for _ in terms],
        ),
        out_shape=[jax.ShapeDtypeStruct((piece, d), BF) for _ in terms],
        compiler_params=pltpu.CompilerParams(vmem_limit_bytes=VMEM),
        cost_estimate=pl.CostEstimate(
            flops=400 * piece * d * len(flat), bytes_accessed=2 * piece * d * len(flat), transcendentals=0),
    )(q4, *[a for a, _ in flat])


def _place_kernel(n, at_ref, *refs):
    src, y_ref, buf, sem = refs[:n], refs[-3], refs[-2], refs[-1]
    piece = buf.shape[1]
    loads = [pltpu.make_async_copy(src[i], buf.at[i], sem.at[0, i]) for i in range(n)]
    for cp in loads:
        cp.start()
    stores = [pltpu.make_async_copy(buf.at[i], y_ref.at[pl.ds(pl.multiple_of(at_ref[i], min(piece, 64)), piece), :], sem.at[1, i])
              for i in range(n)]
    for ld, st in zip(loads, stores):
        ld.wait()
        st.start()
    for st in stores:
        st.wait()


def _place(y, at, pieces, t):
    n = len(pieces)
    piece, d = pieces[0].shape
    extra = [] if y is None else [y]
    any_ = pl.BlockSpec(memory_space=pl.ANY)
    return pl.pallas_call(
        functools.partial(_place_kernel, n),
        grid_spec=pltpu.PrefetchScalarGridSpec(
            num_scalar_prefetch=1,
            grid=(),
            in_specs=[any_] * (n + len(extra)),
            out_specs=any_,
            scratch_shapes=[pltpu.VMEM((n, piece, d), BF), pltpu.SemaphoreType.DMA((2, n))],
        ),
        out_shape=jax.ShapeDtypeStruct((t, d), BF),
        input_output_aliases={n + 1: 0} if extra else {},
        compiler_params=pltpu.CompilerParams(vmem_limit_bytes=VMEM),
        cost_estimate=pl.CostEstimate(flops=800 * n * piece * d, bytes_accessed=4 * n * piece * d, transcendentals=0),
    )(at, *pieces, *extra)


def solution(mesh):
    tp = mesh.shape["tp"]
    assert tp == 8

    def swap(a, bit):
        return lax.ppermute(a, "tp", [(i, i ^ bit) for i in range(tp)])

    core, xs, ys = 1, 2, 4

    def layer(x, pos, g1, g2, wq, wk, wv, wo, wg, wu, wd):
        t, _ = x.shape
        hl = wq.shape[1] // HEAD
        r = lax.axis_index("tp")
        c, q4 = r % 2, r // 2
        chunks = CHUNKS if sum(CHUNKS) == t else tuple(s * t // 8192 for s in CHUNKS)
        q0s = [sum(chunks[:n]) for n in range(len(chunks))]
        qs = jnp.stack([q4 ^ k for k in range(4)])

        m = wo.shape[0] // 2
        w2, w4 = swap(wo, xs), swap(wo, ys)
        w6a, w6b = swap(w2[:m], ys), swap(w4[m:], xs)
        ws = [wo, w2, w4, w6a, w6b]
        wp = [swap(w, core) for w in ws]
        wall = [ws[0], wp[0], ws[1], wp[1], ws[2], wp[2], ws[3], ws[4], wp[3], wp[4]]

        wk_l = lax.dynamic_slice_in_dim(wk, r * HEAD, HEAD, axis=1)
        wv_l = lax.dynamic_slice_in_dim(wv, r * HEAD, HEAD, axis=1)
        cos, sin = _cs(pos)
        q, k, v = _qkv(x, g1, jnp.concatenate([wq, wk_l, wv_l], axis=1), cos, sin, hl)
        kt = k.T

        y = None
        for n, rows in enumerate(chunks):
            half, piece = rows // 2, rows // 8
            o = _attn(q, kt, v, hl, q0s[n], rows)
            oa = lax.dynamic_slice_in_dim(o, c * half, half, axis=0)
            ob = swap(lax.dynamic_slice_in_dim(o, (1 - c) * half, half, axis=0), core)
            oax, oay = swap(oa, xs), swap(oa, ys)
            obx, oby = swap(ob, xs), swap(ob, ys)
            oad, obd = swap(oax, ys), swap(oby, xs)
            h, b = _h(q0s[n] + c * half, x, g2, [oa, ob, oax, obx, oay, oby, oad, obd], wall)
            p0 = _mlp(b, wg, wu, wd)
            p1 = _mlp(swap(b, core), wg, wu, wd)
            p1 = swap(p1, core)

            one, two = (1, 2) if n % 2 == 0 else (2, 1)
            via = {1: xs, 2: ys}
            f, g1st = _sums(qs, piece, [[(p0, 3), (p1, 3)], [(p0, one), (p1, one)]])
            f, g1st = swap(f, via[one]), swap(g1st, via[one])
            g2nd, = _sums(qs, piece, [[(p0, two), (p1, two), (f, None)]])
            g2nd = swap(g2nd, via[two])
            own, = _sums(qs, piece,
                          [[(p0, 0), (p1, 0), (g1st, None), (g2nd, None), (h, 0)]])
            got1, got2 = swap(own, via[one]), swap(own, via[two])
            got3 = swap(got1, via[two])
            mine = [own, got1, got2, got3]
            pieces = mine + [swap(s, core) for s in mine]
            at = jnp.stack([q0s[n] + cc * half + (q4 ^ kk) * piece for cc in (c, 1 - c) for kk in (0, one, two, 3)])
            y = _place(y, at, pieces, t)
        return y, k.reshape(t, 1, HEAD), v.reshape(t, 1, HEAD)

    return jax.shard_map(
        layer,
        mesh=mesh,
        in_specs=(P("dp", None), P("dp"), P(), P(), P(None, "tp"), P(), P(), P("tp", None),
                  P(None, "tp"), P(None, "tp"), P("tp", None)),
        out_specs=(P("dp", None), P("dp", "tp", None), P("dp", "tp", None)),
        check_vma=False,
    )
```

```python
import functools

import jax
import jax.numpy as jnp
from jax import lax
from jax.experimental import pallas as pl
from jax.experimental.pallas import tpu as pltpu
from jax.sharding import PartitionSpec as P


HEAD = 128
EPS = 1e-5
ROPE_BASE = 500000.0
LOG2E = 1.4426950408889634
CHUNKS = (2048, 2048, 2048, 1024, 1024)
VMEM = 62 << 20
F32, BF = jnp.float32, jnp.bfloat16


def _cs(pos):
    half = HEAD // 2
    inv = ROPE_BASE ** (-2.0 * jnp.arange(half, dtype=F32) / HEAD)
    p = pos.astype(F32).reshape(2, -1, 1)
    low = lax.broadcasted_iota(jnp.int32, (1, HEAD), 1) < half
    ang = jnp.where(low, p[0], p[1]) * jnp.tile(inv, 2)
    return jnp.cos(ang), jnp.sin(ang)


def _qkv_kernel(hl, x_ref, g_ref, w_ref, c_ref, s_ref, q_ref, k_ref, v_ref):
    x = x_ref[...].astype(F32)
    inv = lax.rsqrt(jnp.mean(x * x, axis=-1, keepdims=True) + EPS)
    a = (x * inv * g_ref[...].astype(F32)).astype(BF)
    r = jnp.dot(a, w_ref[...], preferred_element_type=F32)
    low = lax.broadcasted_iota(jnp.int32, c_ref.shape, 1) < HEAD // 2
    first = pl.program_id(0) < pl.num_programs(0) // 2
    here = jnp.logical_xor(low, jnp.logical_not(first))

    def both(ref):
        t = ref[...]
        return jnp.where(here, t, pltpu.roll(t, HEAD // 2, 1))

    cc, ss = both(c_ref), both(s_ref)
    ss = jnp.where(low, -ss, ss)
    for n in range(hl + 1):
        t = r[:, n * HEAD:(n + 1) * HEAD]
        t = (t * cc + pltpu.roll(t, HEAD // 2, 1) * ss).astype(BF)
        if n < hl:
            q_ref[:, n * HEAD:(n + 1) * HEAD] = t
        else:
            k_ref[...] = t
    v_ref[...] = r[:, (hl + 1) * HEAD:].astype(BF)


def _qkv(x, g1, w, c, s, hl):
    t, d = x.shape
    bm = min(t // 2, 512)
    nb = t // 2 // bm
    n = w.shape[1]
    row = lambda i: (i, 0)
    fix = lambda i: (0, 0)
    return pl.pallas_call(
        functools.partial(_qkv_kernel, hl),
        grid=(t // bm,),
        in_specs=[
            pl.BlockSpec((bm, d), row),
            pl.BlockSpec((1, d), fix),
            pl.BlockSpec((d, n), fix),
            pl.BlockSpec((bm, HEAD), lambda i: (i % nb, 0)),
            pl.BlockSpec((bm, HEAD), lambda i: (i % nb, 0)),
        ],
        out_specs=[
            pl.BlockSpec((bm, hl * HEAD), row),
            pl.BlockSpec((bm, HEAD), row),
            pl.BlockSpec((bm, HEAD), row),
        ],
        out_shape=[
            jax.ShapeDtypeStruct((t, hl * HEAD), BF),
            jax.ShapeDtypeStruct((t, HEAD), BF),
            jax.ShapeDtypeStruct((t, HEAD), BF),
        ],
        compiler_params=pltpu.CompilerParams(vmem_limit_bytes=VMEM),
        cost_estimate=pl.CostEstimate(flops=2 * t * d * n, bytes_accessed=2 * t * d, transcendentals=0),
        name="qkv",
    )(x, g1.reshape(1, d), w, c, s)


def _attn_kernel(hl, q0, bq, bk, q_ref, kt_ref, v_ref, o_ref, m_sc, l_sc, a_sc):
    i = pl.program_id(0)
    row0 = q0 + i * bq
    c = HEAD ** -0.5 * LOG2E
    for h in range(hl):
        m_sc[h] = jnp.full((bq, HEAD), -1e30, F32)
        l_sc[h] = jnp.zeros((bq, HEAD), F32)
        a_sc[h] = jnp.zeros((bq, HEAD), F32)

    def block(j, masked):
        start = pl.multiple_of(j * bk, bk)
        kt = kt_ref[:, pl.ds(start, bk)]
        v = v_ref[pl.ds(start, bk), :]
        scores = []
        for h in range(hl):
            q = q_ref[:, h * HEAD:(h + 1) * HEAD]
            s = jnp.dot(q, kt, preferred_element_type=F32) * c
            if masked:
                rows = row0 + lax.broadcasted_iota(jnp.int32, (bq, bk), 0)
                cols = start + lax.broadcasted_iota(jnp.int32, (bq, bk), 1)
                s = jnp.where(cols <= rows, s, -jnp.inf)
            scores.append(s)
        for h in range(hl):
            s = scores[h]
            m0 = m_sc[h]
            m1 = jnp.maximum(m0, jnp.max(s, axis=-1, keepdims=True))
            p = jnp.exp2(s - jnp.concatenate([m1] * (bk // HEAD), axis=-1))
            al = jnp.exp2(m0 - m1)
            part = p[:, :HEAD]
            for g in range(1, bk // HEAD):
                part = part + p[:, g * HEAD:(g + 1) * HEAD]
            l_sc[h] = l_sc[h] * al + part
            a_sc[h] = a_sc[h] * al + jnp.dot(p.astype(BF), v, preferred_element_type=F32)
            m_sc[h] = m1

    nfull = row0 // bk

    def body(j, carry):
        block(j, False)
        return carry

    lax.fori_loop(0, nfull, body, 0)
    block(nfull, True)
    for h in range(hl):
        l = jnp.sum(l_sc[h], axis=-1, keepdims=True)
        o_ref[:, h * HEAD:(h + 1) * HEAD] = (a_sc[h] / l).astype(BF)


def _attn(q, kt, v, hl, q0, rows):
    t = v.shape[0]
    bq = min(rows, 512)
    bk = bq
    nq = rows // bq
    b0 = q0 // bq
    end = q0 + rows
    area = sum((q0 + (i + 1) * bq) * bq for i in range(nq))
    return pl.pallas_call(
        functools.partial(_attn_kernel, hl, q0, bq, bk),
        grid=(nq,),
        in_specs=[
            pl.BlockSpec((bq, hl * HEAD), lambda i: (b0 + i, 0)),
            pl.BlockSpec((HEAD, t), lambda i: (0, 0)),
            pl.BlockSpec((t, HEAD), lambda i: (0, 0)),
        ],
        out_specs=pl.BlockSpec((bq, hl * HEAD), lambda i: (i, 0)),
        out_shape=jax.ShapeDtypeStruct((rows, hl * HEAD), BF),
        scratch_shapes=[pltpu.VMEM((hl, bq, HEAD), F32)] * 3,
        compiler_params=pltpu.CompilerParams(vmem_limit_bytes=40 << 20),
        cost_estimate=pl.CostEstimate(
            flops=4 * 3 * HEAD * hl * area, bytes_accessed=4 * end * HEAD, transcendentals=hl * area),
    )(q, kt, v)


def _h_kernel(n, sizes, off_ref, x_ref, g_ref, *refs):
    o_refs, w_refs = refs[:n], refs[n:n + len(sizes)]
    h_ref, b_ref, w_sc, sem = refs[n + len(sizes):]

    @pl.when(pl.program_id(0) == 0)
    def _():
        copies, at = [], 0
        for i, (w, size) in enumerate(zip(w_refs, sizes)):
            copies.append(pltpu.make_async_copy(w, w_sc.at[pl.ds(at, size), :], sem.at[i]))
            at += size
        for cp in copies:
            cp.start()
        for cp in copies:
            cp.wait()

    o = jnp.concatenate([r[...] for r in o_refs], axis=-1)
    h = (x_ref[...].astype(F32) + jnp.dot(o, w_sc[...], preferred_element_type=F32)).astype(BF)
    h_ref[...] = h
    h = h.astype(F32)
    inv = lax.rsqrt(jnp.mean(h * h, axis=-1, keepdims=True) + EPS)
    b_ref[...] = (h * inv * g_ref[...].astype(F32)).astype(BF)


def _h(start, x, g2, os, ws):
    rows, kk = os[0].shape
    d = x.shape[1]
    n = len(os)
    bm = min(rows, 256)
    sizes = tuple(w.shape[0] for w in ws)
    row = lambda i, o: (i, 0)
    fix = lambda i, o: (0, 0)
    return pl.pallas_call(
        functools.partial(_h_kernel, n, sizes),
        grid_spec=pltpu.PrefetchScalarGridSpec(
            num_scalar_prefetch=1,
            grid=(rows // bm,),
            in_specs=[
                pl.BlockSpec((bm, d), lambda i, o: (o[0] + i, 0)),
                pl.BlockSpec((1, d), fix),
                *[pl.BlockSpec((bm, kk), row) for _ in range(n)],
                *[pl.BlockSpec(memory_space=pl.ANY) for _ in ws],
            ],
            out_specs=[pl.BlockSpec((bm, d), row), pl.BlockSpec((bm, d), row)],
            scratch_shapes=[pltpu.VMEM((n * kk, d), BF), pltpu.SemaphoreType.DMA((len(ws),))],
        ),
        out_shape=[jax.ShapeDtypeStruct((rows, d), BF)] * 2,
        compiler_params=pltpu.CompilerParams(vmem_limit_bytes=VMEM),
        cost_estimate=pl.CostEstimate(
            flops=2 * rows * d * n * kk, bytes_accessed=2 * d * (n * kk + 4 * rows), transcendentals=0),
    )((start // bm).reshape(1), x, g2.reshape(1, d), *os, *ws)


def _mlp_kernel(fb, db, b_ref, wg_ref, wu_ref, wd_ref, p_ref, wg_sc, wu_sc, wd_sc, u_sc, sem):
    d, f = wg_sc.shape
    first = pl.program_id(0) == 0

    def up_copies(j):
        cols = pl.ds(j * fb, fb)
        return (pltpu.make_async_copy(wg_ref.at[:, cols], wg_sc.at[:, cols], sem.at[0, j]),
                pltpu.make_async_copy(wu_ref.at[:, cols], wu_sc.at[:, cols], sem.at[1, j]))

    def down_copy():
        return pltpu.make_async_copy(wd_ref, wd_sc, sem.at[2, 0])

    @pl.when(first)
    def _():
        for j in range(f // fb):
            for cp in up_copies(j):
                cp.start()
        down_copy().start()

    b = b_ref[...]
    for j in range(f // fb):
        @pl.when(first)
        def _():
            for cp in up_copies(j):
                cp.wait()

        cols = slice(j * fb, (j + 1) * fb)
        gt = jnp.dot(b, wg_sc[:, cols], preferred_element_type=F32)
        up = jnp.dot(b, wu_sc[:, cols], preferred_element_type=F32)
        u_sc[:, cols] = (gt * jax.nn.sigmoid(gt) * up).astype(BF)

    @pl.when(first)
    def _():
        down_copy().wait()

    u = u_sc[...]
    for j in range(d // db):
        cols = slice(j * db, (j + 1) * db)
        p_ref[:, cols] = jnp.dot(u, wd_sc[:, cols], preferred_element_type=F32).astype(BF)


def _mlp(b, wg, wu, wd):
    rows, d = b.shape
    f = wg.shape[1]
    bm = next((m for m in (512, 384, 256) if rows % m == 0), rows)
    fb, db = min(f, 512), min(d, 512)
    row = lambda i: (i, 0)
    any_ = pl.BlockSpec(memory_space=pl.ANY)
    return pl.pallas_call(
        functools.partial(_mlp_kernel, fb, db),
        grid=(rows // bm,),
        in_specs=[pl.BlockSpec((bm, d), row), any_, any_, any_],
        out_specs=pl.BlockSpec((bm, d), row),
        out_shape=jax.ShapeDtypeStruct((rows, d), BF),
        scratch_shapes=[pltpu.VMEM((d, f), BF), pltpu.VMEM((d, f), BF), pltpu.VMEM((f, d), BF),
                        pltpu.VMEM((bm, f), BF), pltpu.SemaphoreType.DMA((3, f // fb))],
        compiler_params=pltpu.CompilerParams(vmem_limit_bytes=VMEM),
        cost_estimate=pl.CostEstimate(
            flops=6 * rows * d * f, bytes_accessed=2 * d * (3 * f + 2 * rows), transcendentals=rows * f),
    )(b, wg, wu, wd)


def _sum_kernel(groups, q_ref, *refs):
    at = 0
    outs = refs[sum(groups):]
    for g, out in zip(groups, outs):
        t = refs[at][...].astype(F32)
        for r in refs[at + 1:at + g]:
            t = t + r[...].astype(F32)
        out[...] = t.astype(BF)
        at += g


def _sums(q4, piece, terms):
    d = terms[0][0][0].shape[1]
    bm = min(piece, 64)
    nb = piece // bm
    own = lambda i, q: (i, 0)

    def spec(k):
        if k is None:
            return pl.BlockSpec((bm, d), own)
        return pl.BlockSpec((bm, d), lambda i, q: (q[k] * nb + i, 0))

    flat = [t for group in terms for t in group]
    return pl.pallas_call(
        functools.partial(_sum_kernel, tuple(len(g) for g in terms)),
        grid_spec=pltpu.PrefetchScalarGridSpec(
            num_scalar_prefetch=1,
            grid=(nb,),
            in_specs=[spec(k) for _, k in flat],
            out_specs=[pl.BlockSpec((bm, d), own) for _ in terms],
        ),
        out_shape=[jax.ShapeDtypeStruct((piece, d), BF) for _ in terms],
        compiler_params=pltpu.CompilerParams(vmem_limit_bytes=VMEM),
        cost_estimate=pl.CostEstimate(
            flops=400 * piece * d * len(flat), bytes_accessed=2 * piece * d * len(flat), transcendentals=0),
    )(q4, *[a for a, _ in flat])


def _place_kernel(n, at_ref, *refs):
    src, y_ref, buf, sem = refs[:n], refs[-3], refs[-2], refs[-1]
    piece = buf.shape[1]
    loads = [pltpu.make_async_copy(src[i], buf.at[i], sem.at[0, i]) for i in range(n)]
    for cp in loads:
        cp.start()
    stores = [pltpu.make_async_copy(buf.at[i], y_ref.at[pl.ds(pl.multiple_of(at_ref[i], min(piece, 64)), piece), :], sem.at[1, i])
              for i in range(n)]
    for ld, st in zip(loads, stores):
        ld.wait()
        st.start()
    for st in stores:
        st.wait()


def _place(y, at, pieces, t):
    n = len(pieces)
    piece, d = pieces[0].shape
    extra = [] if y is None else [y]
    any_ = pl.BlockSpec(memory_space=pl.ANY)
    return pl.pallas_call(
        functools.partial(_place_kernel, n),
        grid_spec=pltpu.PrefetchScalarGridSpec(
            num_scalar_prefetch=1,
            grid=(),
            in_specs=[any_] * (n + len(extra)),
            out_specs=any_,
            scratch_shapes=[pltpu.VMEM((n, piece, d), BF), pltpu.SemaphoreType.DMA((2, n))],
        ),
        out_shape=jax.ShapeDtypeStruct((t, d), BF),
        input_output_aliases={n + 1: 0} if extra else {},
        compiler_params=pltpu.CompilerParams(vmem_limit_bytes=VMEM),
        cost_estimate=pl.CostEstimate(flops=800 * n * piece * d, bytes_accessed=4 * n * piece * d, transcendentals=0),
    )(at, *pieces, *extra)


def solution(mesh):
    tp = mesh.shape["tp"]
    assert tp == 8

    def swap(a, bit):
        return lax.ppermute(a, "tp", [(i, i ^ bit) for i in range(tp)])

    core, xs, ys = 1, 2, 4

    def layer(x, pos, g1, g2, wq, wk, wv, wo, wg, wu, wd):
        t, _ = x.shape
        hl = wq.shape[1] // HEAD
        r = lax.axis_index("tp")
        c, q4 = r % 2, r // 2
        chunks = CHUNKS if sum(CHUNKS) == t else tuple(s * t // 8192 for s in CHUNKS)
        q0s = [sum(chunks[:n]) for n in range(len(chunks))]
        qs = jnp.stack([q4 ^ k for k in range(4)])

        m = wo.shape[0] // 2
        w2, w4 = swap(wo, xs), swap(wo, ys)
        w6a, w6b = swap(w2[:m], ys), swap(w4[m:], xs)
        ws = [wo, w2, w4, w6a, w6b]
        wp = [swap(w, core) for w in ws]
        wall = [ws[0], wp[0], ws[1], wp[1], ws[2], wp[2], ws[3], ws[4], wp[3], wp[4]]

        wk_l = lax.dynamic_slice_in_dim(wk, r * HEAD, HEAD, axis=1)
        wv_l = lax.dynamic_slice_in_dim(wv, r * HEAD, HEAD, axis=1)
        cos, sin = _cs(pos)
        q, k, v = _qkv(x, g1, jnp.concatenate([wq, wk_l, wv_l], axis=1), cos, sin, hl)
        kt = k.T

        y = None
        for n, rows in enumerate(chunks):
            half, piece = rows // 2, rows // 8
            o = _attn(q, kt, v, hl, q0s[n], rows)
            oa = lax.dynamic_slice_in_dim(o, c * half, half, axis=0)
            ob = swap(lax.dynamic_slice_in_dim(o, (1 - c) * half, half, axis=0), core)
            oax, oay = swap(oa, xs), swap(oa, ys)
            obx, oby = swap(ob, xs), swap(ob, ys)
            oad, obd = swap(oax, ys), swap(oby, xs)
            h, b = _h(q0s[n] + c * half, x, g2, [oa, ob, oax, obx, oay, oby, oad, obd], wall)
            p0 = _mlp(b, wg, wu, wd)
            p1 = _mlp(swap(b, core), wg, wu, wd)
            p1 = swap(p1, core)

            one, two = (1, 2) if n % 2 == 0 else (2, 1)
            via = {1: xs, 2: ys}
            f, g1st = _sums(qs, piece, [[(p0, 3), (p1, 3)], [(p0, one), (p1, one)]])
            f, g1st = swap(f, via[one]), swap(g1st, via[one])
            g2nd, = _sums(qs, piece, [[(p0, two), (p1, two), (f, None)]])
            g2nd = swap(g2nd, via[two])
            own, = _sums(qs, piece,
                          [[(p0, 0), (p1, 0), (g1st, None), (g2nd, None), (h, 0)]])
            got1, got2 = swap(own, via[one]), swap(own, via[two])
            got3 = swap(got1, via[two])
            mine = [own, got1, got2, got3]
            pieces = mine + [swap(s, core) for s in mine]
            at = jnp.stack([q0s[n] + cc * half + (q4 ^ kk) * piece for cc in (c, 1 - c) for kk in (0, one, two, 3)])
            y = _place(y, at, pieces, t)
        return y, k.reshape(t, 1, HEAD), v.reshape(t, 1, HEAD)

    return jax.shard_map(
        layer,
        mesh=mesh,
        in_specs=(P("dp", None), P("dp"), P(), P(), P(None, "tp"), P(), P(), P("tp", None),
                  P(None, "tp"), P(None, "tp"), P("tp", None)),
        out_specs=(P("dp", None), P("dp", "tp", None), P("dp", "tp", None)),
        check_vma=False,
    )
```
